32 devices in a mesh: seg: 4 (over y, x), lat: 8 (over z, core).
Axes of the slice: x: 2, y: 2, z: 4, core: 2. Of those that a mesh axis runs over, the one named last changes fastest.
Arguments:
- coh_map: bfloat16 [4, 65536, 128], P('seg', 'lat'), may hold values from 0 to 40, as said below
- positions: int32 [4, 1024], P('seg', 'lat'), may hold values from 0 to 16776959, as said below
- counts: int32 [16], P('lat'), may hold values from 1 to 64, as said below
Outputs:
- semi_stat: bfloat16 [1024, 128], P('lat')
- excess: float32 [16, 128], P('lat')
The draws below stay inside these ranges and needn't reach their ends.
Inputs may be any that keep to these rules, and one draw needn't show every extreme that they name: `coh_map`: nonnegative. `counts`: the first block has 1 valid point and the last block 64. `positions`: the bins are split into 8 aligned slices of 8192 bins; a point's two bins lie in the same slice; in each segment, at most 32 of the 128 points of one index of lat have their bins in one slice, and that most is reached in every draw.
All inputs are finite; a program needn't handle non-finite values.
Results may differ from the reference program's by a relative error of at most 0.001.
Values sent between devices are 32-bit elements; how exact they have to be, the bound alone decides.
A program may use at most 64 MiB of HBM per device.

```python
import math
import jax
import jax.numpy as jnp
from jax import lax

F = 65536
NSD = 128
BLK = 64
PT_DEV = 128
S = 4
NB = 16
SLICE = 8192
N_LAT = 8


def draw_coh_map(key, part):
    first_key, second_key, third_key = jax.random.split(jax.random.fold_in(key, 11), 3)
    column_scale = jnp.exp(jax.random.uniform(third_key, (NSD,), jnp.float32, math.log(0.1), 0.0))
    values = 2.0 * (jax.random.exponential(first_key, (S, F, NSD), jnp.float32) + jax.random.exponential(second_key, (S, F, NSD), jnp.float32))
    return jnp.clip(values * column_scale, 0.0, 40.0).astype(jnp.bfloat16)


def draw_positions(key, part):
    base_key = jax.random.fold_in(key, 37)
    perm_key, split_key, shuffle_key, bin_key, frac_key = jax.random.split(base_key, 5)
    pair_total = N_LAT // 2
    slot_limit = 2 * PT_DEV // N_LAT
    dest_scores = jax.random.randint(perm_key, (S, N_LAT, N_LAT), 0, 1 << 20, dtype=jnp.int32) * N_LAT + jnp.arange(N_LAT, dtype=jnp.int32)
    dest_perm = jnp.argsort(dest_scores, axis=-1, stable=True).astype(jnp.int32)
    split_at = jax.random.randint(split_key, (S, N_LAT, pair_total), 0, slot_limit + 1, dtype=jnp.int32)
    split_at = split_at.at[:, :, 0].set(slot_limit)
    point_ids = jnp.arange(PT_DEV, dtype=jnp.int32)
    pair_ids = point_ids // slot_limit
    within = point_ids % slot_limit
    split_points = jnp.take(split_at, pair_ids, axis=2)
    first_dest = jnp.take(dest_perm, 2 * pair_ids, axis=2)
    second_dest = jnp.take(dest_perm, 2 * pair_ids + 1, axis=2)
    dest = jnp.where(within[None, None, :] < split_points, first_dest, second_dest)
    point_scores = jax.random.randint(shuffle_key, (S, N_LAT, PT_DEV), 0, 1 << 20, dtype=jnp.int32) * PT_DEV + point_ids
    shuffle = jnp.argsort(point_scores, axis=-1, stable=True).astype(jnp.int32)
    dest = jnp.take_along_axis(dest, shuffle, axis=-1)
    low_bin = dest * SLICE + jax.random.randint(bin_key, (S, N_LAT, PT_DEV), 0, SLICE - 1, dtype=jnp.int32)
    drawn = low_bin * 256 + jax.random.randint(frac_key, (S, N_LAT, PT_DEV), 0, 256, dtype=jnp.int32)
    return drawn.reshape(S, N_LAT * PT_DEV).astype(jnp.int32)


def draw_counts(key, part):
    block_id = jnp.arange(NB, dtype=jnp.int32)
    low_bound = 1 + BLK // 2 * block_id // NB
    high_bound = 1 + BLK // 4 + 3 * BLK // 4 * block_id // NB
    raw_bits = jax.random.randint(jax.random.fold_in(key, 23), (NB,), 0, 1 << 20, dtype=jnp.int32)
    drawn = low_bound + raw_bits % (high_bound - low_bound)
    drawn = drawn.at[0].set(1).at[NB - 1].set(BLK)
    return drawn.astype(jnp.int32)


def setup_inputs(seed: int = 0) -> dict:
    key_list = jax.random.split(jax.random.key(seed), 4)
    coh_map = draw_coh_map(jax.random.fold_in(key_list[3], 71), 0)
    positions = draw_positions(jax.random.fold_in(key_list[3], 71), 0)
    counts = draw_counts(jax.random.fold_in(key_list[3], 71), 0)
    return {"coh_map": coh_map, "positions": positions, "counts": counts}


def reference(coh_map, positions, counts):
    low_bin = positions // 256
    fraction = (positions % 256).astype(jnp.float32) / 256.0

    def accumulate(running, inputs):
        seg_map, low_index, weight_hi = inputs
        near_rows = jnp.take(seg_map, low_index, axis=0).astype(jnp.float32)
        far_rows = jnp.take(seg_map, low_index + 1, axis=0).astype(jnp.float32)
        running = running + (1.0 - weight_hi)[:, None] * near_rows + weight_hi[:, None] * far_rows
        return running, None

    start_sum = jnp.zeros((positions.shape[1], coh_map.shape[2]), jnp.float32)
    summed, _ = lax.scan(accumulate, start_sum, (coh_map, low_bin, fraction))
    semi_stat = summed / coh_map.shape[0]
    grouped = semi_stat.reshape(NB, BLK, NSD)
    slot_index = lax.broadcasted_iota(jnp.int32, (NB, BLK, 1), 1)
    live_mask = slot_index < counts[:, None, None]
    block_sum = jnp.sum(jnp.where(live_mask, grouped, 0.0), axis=1)
    count_float = counts.astype(jnp.float32)
    block_mean = block_sum / count_float[:, None]
    global_mean = jnp.sum(block_sum, axis=0) / jnp.sum(count_float)
    excess = block_mean - global_mean[None, :]
    return semi_stat.astype(jnp.bfloat16), excess
```

```python
import functools

import jax
import jax.numpy as jnp
from jax import lax
from jax.experimental import pallas as pl
from jax.experimental.pallas import tpu as pltpu
from jax.sharding import PartitionSpec as P

MESH = pl.DeviceIdType.MESH
PIECES = 4


def kernel(
    n_lat,
    n_seg,
    pos_ref,
    cnt_ref,
    coh_hbm,
    semi_ref,
    excess_ref,
    coh,
    gath,
    rows_out,
    rows_in,
    col_out,
    col_in,
    part,
    part_in,
    psum,
    psum_in,
    coh_sem,
    gs_sem,
    gr_sem,
    rs_sem,
    rr_sem,
    cs_sem,
    cr_sem,
    xs_sem,
    xr_sem,
):
    lat = lax.axis_index("lat")
    seg = lax.axis_index("seg")
    slice_bins, width = coh.shape
    points = pos_ref.shape[1]
    blocks = cnt_ref.shape[0]
    block_size = points // blocks
    slots = 2 * points // n_lat
    total_slots = n_lat * slots
    steps = n_seg.bit_length() - 1
    f32, bf16, i32 = jnp.float32, jnp.bfloat16, jnp.int32

    piece = slice_bins // PIECES
    loads = []
    for k in range(PIECES):
        rng = pl.ds(k * piece, piece)
        loads.append(pltpu.make_async_copy(coh_hbm.at[0, rng], coh.at[rng], coh_sem.at[k]))
        loads[-1].start()

    barrier = pltpu.get_barrier_semaphore()
    lat_peers = [lax.rem(lat + j, n_lat) for j in range(n_lat)]
    lat_back = [lax.rem(lat + n_lat - j, n_lat) for j in range(n_lat)]
    seg_peers = []
    for b in range(steps):
        w = 1 << b
        bit = lax.rem(seg // w, 2)
        seg_peers.append(seg + w - 2 * w * bit)
    for j in range(1, n_lat):
        pl.semaphore_signal(barrier, inc=1, device_id=(seg, lat_peers[j]), device_id_type=MESH)
    for b in range(steps):
        pl.semaphore_signal(barrier, inc=1, device_id=(seg_peers[b], lat), device_id_type=MESH)

    pos = pos_ref[...]
    lane = lax.broadcasted_iota(i32, (1, points), 1)
    dest = (pos // 256) // slice_bins
    rel = lax.rem(dest - lat + n_lat, n_lat)
    hits = lax.broadcasted_iota(i32, (n_lat, points), 0) == rel
    hits_f = hits.astype(f32)
    tri = (
        lax.broadcasted_iota(i32, (points, points), 0)
        < lax.broadcasted_iota(i32, (points, points), 1)
    ).astype(f32)
    before = jnp.dot(hits_f.astype(bf16), tri.astype(bf16), preferred_element_type=f32)
    slot = jnp.sum(before * hits_f, axis=0, keepdims=True).astype(i32)
    sid = rel * slots + slot
    limit = jnp.zeros((1, points), i32)
    for b in range(blocks):
        limit = jnp.where(lane // block_size == b, cnt_ref[b], limit)
    valid = (lane % block_size < limit).astype(i32)
    gath[0, 0:1, :] = sid
    gath[0, 1:2, :] = pos
    gath[0, 2:3, :] = valid
    gath[0, 3:4, :] = valid

    pl.semaphore_wait(barrier, n_lat - 1 + steps)
    sends = []
    for j in range(1, n_lat):
        copy = pltpu.make_async_remote_copy(
            src_ref=gath.at[0],
            dst_ref=gath.at[j],
            send_sem=gs_sem.at[j],
            recv_sem=gr_sem.at[j],
            device_id=(seg, lat_peers[j]),
            device_id_type=MESH,
        )
        copy.start()
        sends.append(copy)

    pick_t = (lax.broadcasted_iota(i32, (total_slots, points), 0) == sid).astype(f32)
    pick = pick_t.T.astype(bf16)

    for copy in sends:
        copy.wait_recv()

    base = lat * (slice_bins * 256)
    flag = slice_bins * 256
    sub = lax.broadcasted_iota(i32, (slots, points), 0)
    cols = []
    count = jnp.zeros((1, points), i32)
    for j in range(n_lat):
        code = (gath[j, 1:2, :] - base + flag * (1 + gath[j, 2:3, :])).astype(f32)
        here = (gath[j, 0:1, :] - j * slots) == sub
        cols.append(jnp.sum(jnp.where(here, code, 0.0), axis=1, keepdims=True))
        count = count + gath[j, 2:3, :]
    code = jnp.concatenate(cols, axis=0).astype(i32)
    total_count = jnp.sum(count.astype(f32), axis=1, keepdims=True)
    present = code >= flag
    live = code >= 2 * flag
    off = code % flag
    low = off // 256
    upper = (off % 256).astype(f32) / 256.0
    depth = min(256, slice_bins)
    chunk = low // depth
    in_chunk = low % depth
    bins = lax.broadcasted_iota(i32, (total_slots, depth), 1)
    local = jnp.where(bins == in_chunk, 1.0 - upper, 0.0) + jnp.where(
        bins == (in_chunk + 1) % depth, upper, 0.0
    )
    where_id = jnp.where(bins < in_chunk, chunk + 1, chunk)
    where_id = jnp.where(present, where_id, -1)
    local = local.astype(bf16)
    where_id = where_id.astype(f32).astype(bf16)
    zero = jnp.zeros_like(local)

    held = jnp.zeros((total_slots, width), f32)
    per_piece = piece // depth
    for k in range(PIECES):
        loads[k].wait()
        weights = jnp.concatenate(
            [
                jnp.where(where_id == jnp.asarray(k * per_piece + c, bf16), local, zero)
                for c in range(per_piece)
            ],
            axis=1,
        )
        held = held + jnp.dot(
            weights, coh[k * piece : (k + 1) * piece, :], preferred_element_type=f32
        )

    col = jnp.sum(jnp.where(live, held, 0.0), axis=0, keepdims=True)
    for j in range(n_lat):
        rows_out[j] = held[j * slots : (j + 1) * slots, :]
    col_out[...] = col
    back = []
    for j in range(1, n_lat):
        copy = pltpu.make_async_remote_copy(
            src_ref=rows_out.at[j],
            dst_ref=rows_in.at[j],
            send_sem=rs_sem.at[j],
            recv_sem=rr_sem.at[j],
            device_id=(seg, lat_back[j]),
            device_id_type=MESH,
        )
        copy.start()
        back.append(copy)
        copy = pltpu.make_async_remote_copy(
            src_ref=col_out,
            dst_ref=col_in.at[j],
            send_sem=cs_sem.at[j],
            recv_sem=cr_sem.at[j],
            device_id=(seg, lat_back[j]),
            device_id_type=MESH,
        )
        copy.start()
        back.append(copy)
    for copy in back:
        copy.wait_recv()

    own = [rows_out[0]] + [rows_in[j] for j in range(1, n_lat)]
    got = jnp.concatenate(own, axis=0)
    high = got.astype(bf16)
    rest = (got - high.astype(f32)).astype(bf16)
    total = jnp.dot(pick, high, preferred_element_type=f32) + jnp.dot(
        pick, rest, preferred_element_type=f32
    )
    for j in range(1, n_lat):
        col = col + col_in[j]

    half = points // 2
    halves = [total[:half], total[half:]]
    outs = []
    for t in range(steps):
        moves = []
        order = (t, steps - 1 - t)
        for h in range(2):
            part[t, h] = halves[h]
        psum[t] = col
        for h in range(2):
            copy = pltpu.make_async_remote_copy(
                src_ref=part.at[t, h],
                dst_ref=part_in.at[t, h],
                send_sem=xs_sem.at[t, h],
                recv_sem=xr_sem.at[t, h],
                device_id=(seg_peers[order[h]], lat),
                device_id_type=MESH,
            )
            copy.start()
            moves.append(copy)
        copy = pltpu.make_async_remote_copy(
            src_ref=psum.at[t],
            dst_ref=psum_in.at[t],
            send_sem=xs_sem.at[t, 2],
            recv_sem=xr_sem.at[t, 2],
            device_id=(seg_peers[order[0]], lat),
            device_id_type=MESH,
        )
        copy.start()
        moves.append(copy)
        for copy in moves:
            copy.wait_recv()
        halves = [halves[h] + part_in[t, h] for h in range(2)]
        col = col + psum_in[t]
        outs += moves

    stat = jnp.concatenate(halves, axis=0) / n_seg
    semi_ref[...] = stat.astype(semi_ref.dtype)
    global_mean = (col / n_seg) / total_count
    row = lax.broadcasted_iota(i32, (block_size, width), 0)
    for b in range(blocks):
        block = stat[b * block_size : (b + 1) * block_size]
        block_sum = jnp.sum(jnp.where(row < cnt_ref[b], block, 0.0), axis=0, keepdims=True)
        mean = block_sum / jnp.full((1, width), cnt_ref[b], i32).astype(f32)
        excess_ref[b : b + 1, :] = mean - global_mean

    for copy in sends + back + outs:
        copy.wait_send()


def shards(n_lat, n_seg, coh_map, positions, counts):
    _, slice_bins, width = coh_map.shape
    points = positions.shape[1]
    blocks = counts.shape[0]
    slots = 2 * points // n_lat
    steps = n_seg.bit_length() - 1
    f32 = jnp.float32
    dma = pltpu.SemaphoreType.DMA
    return pl.pallas_call(
        functools.partial(kernel, n_lat, n_seg),
        out_shape=(
            jax.ShapeDtypeStruct((points, width), jnp.bfloat16),
            jax.ShapeDtypeStruct((blocks, width), f32),
        ),
        in_specs=[
            pl.BlockSpec(memory_space=pltpu.VMEM),
            pl.BlockSpec(memory_space=pltpu.SMEM),
            pl.BlockSpec(memory_space=pl.ANY),
        ],
        out_specs=(
            pl.BlockSpec(memory_space=pltpu.VMEM),
            pl.BlockSpec(memory_space=pltpu.VMEM),
        ),
        scratch_shapes=[
            pltpu.VMEM((slice_bins, width), coh_map.dtype),
            pltpu.VMEM((n_lat, 4, points), jnp.int32),
            pltpu.VMEM((n_lat, slots, width), f32),
            pltpu.VMEM((n_lat, slots, width), f32),
            pltpu.VMEM((1, width), f32),
            pltpu.VMEM((n_lat, 1, width), f32),
            pltpu.VMEM((steps, 2, points // 2, width), f32),
            pltpu.VMEM((steps, 2, points // 2, width), f32),
            pltpu.VMEM((steps, 1, width), f32),
            pltpu.VMEM((steps, 1, width), f32),
            dma((PIECES,)),
            dma((n_lat,)),
            dma((n_lat,)),
            dma((n_lat,)),
            dma((n_lat,)),
            dma((n_lat,)),
            dma((n_lat,)),
            dma((steps, 3)),
            dma((steps, 3)),
        ],
        compiler_params=pltpu.CompilerParams(collective_id=0, has_side_effects=True),
    )(positions, counts, coh_map)


def solution(mesh):
    in_specs = (P("seg", "lat", None), P("seg", "lat"), P("lat"))
    out_specs = (P("lat", None), P("lat", None))
    body = functools.partial(shards, mesh.shape["lat"], mesh.shape["seg"])
    return jax.shard_map(body, mesh=mesh, in_specs=in_specs, out_specs=out_specs, check_vma=False)
```

```python
import functools

import jax
import jax.numpy as jnp
from jax import lax
from jax.experimental import pallas as pl
from jax.experimental.pallas import tpu as pltpu
from jax.sharding import PartitionSpec as P

MESH = pl.DeviceIdType.MESH
PIECES = 4
PARTS = 2
CHUNKS = 4


def flip(index, mask):
    out = index
    w = 1
    while w <= mask:
        if mask & w:
            out = out + w - 2 * w * lax.rem(index // w, 2)
        w *= 2
    return out


def kernel(
    n_lat,
    n_seg,
    pos_hbm,
    cnt_hbm,
    coh_hbm,
    semi_ref,
    excess_ref,
    pos_ref,
    cnt_ref,
    coh,
    gath,
    rows_out,
    rows_in,
    col_out,
    col_in,
    part,
    part_in,
    psum,
    psum_in,
    coh_sem,
    gs_sem,
    gr_sem,
    rs_sem,
    rr_sem,
    cs_sem,
    cr_sem,
    xs_sem,
    xr_sem,
    in_sem,
):
    lat = lax.axis_index("lat")
    seg = lax.axis_index("seg")
    slice_bins, width = coh.shape
    points = pos_ref.shape[1]
    blocks = cnt_ref.shape[0]
    block_size = points // blocks
    slots = 2 * points // n_lat
    total_slots = n_lat * slots
    steps = n_seg.bit_length() - 1
    f32, bf16, i32 = jnp.float32, jnp.bfloat16, jnp.int32

    barrier = pltpu.get_barrier_semaphore()
    lat_peers = [flip(lat, j) for j in range(n_lat)]
    seg_peers = [flip(seg, 1 << b) for b in range(steps)]
    far_first = list(range(n_lat - 1, 0, -1))
    for j in far_first:
        pl.semaphore_signal(barrier, inc=1, device_id=(seg, lat_peers[j]), device_id_type=MESH)
    for b in range(steps):
        pl.semaphore_signal(barrier, inc=1, device_id=(seg_peers[b], lat), device_id_type=MESH)

    small = [
        pltpu.make_async_copy(pos_hbm, pos_ref, in_sem.at[0]),
        pltpu.make_async_copy(cnt_hbm, cnt_ref, in_sem.at[1]),
    ]
    for copy in small:
        copy.start()
    piece = slice_bins // PIECES
    loads = []
    for k in range(PIECES):
        rng = pl.ds(k * piece, piece)
        loads.append(pltpu.make_async_copy(coh_hbm.at[0, rng], coh.at[rng], coh_sem.at[k]))
        loads[-1].start()
    for copy in small:
        copy.wait()

    pos = pos_ref[...]
    lane = lax.broadcasted_iota(i32, (1, points), 1)
    dest = (pos // 256) // slice_bins
    rel = jnp.bitwise_xor(dest, jnp.full((1, points), lat, i32))
    hits = lax.broadcasted_iota(i32, (n_lat, points), 0) == rel
    hits_f = hits.astype(f32)
    tri = (
        lax.broadcasted_iota(i32, (points, points), 0)
        < lax.broadcasted_iota(i32, (points, points), 1)
    ).astype(f32)
    before = jnp.dot(hits_f.astype(bf16), tri.astype(bf16), preferred_element_type=f32)
    slot = jnp.sum(before * hits_f, axis=0, keepdims=True).astype(i32)
    sid = rel * slots + slot
    limit = jnp.zeros((1, points), i32)
    for b in range(blocks):
        limit = jnp.where(lane // block_size == b, cnt_ref[b], limit)
    valid = (lane % block_size < limit).astype(i32)
    gath[0, 0:1, :] = sid
    gath[0, 1:2, :] = pos
    gath[0, 2:3, :] = valid
    gath[0, 3:4, :] = valid

    pl.semaphore_wait(barrier, n_lat - 1 + steps)
    sends = []
    for j in far_first:
        copy = pltpu.make_async_remote_copy(
            src_ref=gath.at[0],
            dst_ref=gath.at[j],
            send_sem=gs_sem.at[j],
            recv_sem=gr_sem.at[j],
            device_id=(seg, lat_peers[j]),
            device_id_type=MESH,
        )
        copy.start()
        sends.append(copy)

    pick_t = (lax.broadcasted_iota(i32, (total_slots, points), 0) == sid).astype(f32)
    pick = pick_t.T.astype(bf16)

    for copy in sends:
        copy.wait_recv()

    base = lat * (slice_bins * 256)
    flag = slice_bins * 256
    sub = lax.broadcasted_iota(i32, (slots, points), 0)
    cols = []
    count = jnp.zeros((1, points), i32)
    for j in range(n_lat):
        code = (gath[j, 1:2, :] - base + flag * (1 + gath[j, 2:3, :])).astype(f32)
        here = (gath[j, 0:1, :] - j * slots) == sub
        cols.append(jnp.sum(jnp.where(here, code, 0.0), axis=1, keepdims=True))
        count = count + gath[j, 2:3, :]
    code = jnp.concatenate(cols, axis=0).astype(i32)
    total_count = jnp.sum(count.astype(f32), axis=1, keepdims=True)
    present = code >= flag
    live = code >= 2 * flag
    off = code % flag
    low = off // 256
    upper = (off % 256).astype(f32) / 256.0
    depth = min(256, slice_bins)
    chunk = low // depth
    in_chunk = low % depth
    bins = lax.broadcasted_iota(i32, (total_slots, depth), 1)
    local = jnp.where(bins == in_chunk, 1.0 - upper, 0.0) + jnp.where(
        bins == (in_chunk + 1) % depth, upper, 0.0
    )
    where_id = jnp.where(bins < in_chunk, chunk + 1, chunk)
    where_id = jnp.where(present, where_id, -1)
    local = local.astype(bf16)
    where_id = where_id.astype(f32).astype(bf16)
    zero = jnp.zeros_like(local)

    per_piece = piece // depth
    back = []
    col = jnp.zeros((1, width), f32)
    group = n_lat // PARTS
    for part_id in range(PARTS - 1, -1, -1):
        lo, hi = part_id * group * slots, (part_id + 1) * group * slots
        held = jnp.zeros((hi - lo, width), f32)
        for k in range(PIECES):
            if part_id == PARTS - 1:
                loads[k].wait()
            weights = jnp.concatenate(
                [
                    jnp.where(
                        where_id[lo:hi] == jnp.asarray(k * per_piece + c, bf16),
                        local[lo:hi],
                        zero[lo:hi],
                    )
                    for c in range(per_piece)
                ],
                axis=1,
            )
            held = held + jnp.dot(
                weights, coh[k * piece : (k + 1) * piece, :], preferred_element_type=f32
            )
        for j in range((part_id + 1) * group - 1, part_id * group - 1, -1):
            rows_out[j] = held[j * slots - lo : (j + 1) * slots - lo, :]
        for j in range((part_id + 1) * group - 1, max(part_id * group, 1) - 1, -1):
            copy = pltpu.make_async_remote_copy(
                src_ref=rows_out.at[j],
                dst_ref=rows_in.at[j],
                send_sem=rs_sem.at[j],
                recv_sem=rr_sem.at[j],
                device_id=(seg, lat_peers[j]),
                device_id_type=MESH,
            )
            copy.start()
            back.append(copy)
        col = col + jnp.sum(jnp.where(live[lo:hi], held, 0.0), axis=0, keepdims=True)
    col_out[...] = col
    for j in far_first:
        copy = pltpu.make_async_remote_copy(
            src_ref=col_out,
            dst_ref=col_in.at[j],
            send_sem=cs_sem.at[j],
            recv_sem=cr_sem.at[j],
            device_id=(seg, lat_peers[j]),
            device_id_type=MESH,
        )
        copy.start()
        back.append(copy)
    for copy in back:
        copy.wait_recv()

    own = [rows_out[0]] + [rows_in[j] for j in range(1, n_lat)]
    got = jnp.concatenate(own, axis=0)
    high = got.astype(bf16)
    rest = (got - high.astype(f32)).astype(bf16)
    total = jnp.dot(pick, high, preferred_element_type=f32) + jnp.dot(
        pick, rest, preferred_element_type=f32
    )
    for j in range(1, n_lat):
        col = col + col_in[j]

    rows = points // CHUNKS
    state = [total[c * rows : (c + 1) * rows] for c in range(CHUNKS)] + [col]
    turn = [c // 2 + (c % 2) * (CHUNKS // 2) for c in range(CHUNKS)] + [CHUNKS]
    outs = []
    arriving = {}
    for t in range(steps + 1):
        for c in turn:
            box, box_in = (part, part_in) if c < CHUNKS else (psum, psum_in)
            at = (c,) if c < CHUNKS else ()
            if t > 0:
                arriving[c].wait_recv()
                state[c] = state[c] + box_in[(t - 1,) + at]
            if t == steps:
                continue
            box[(t,) + at] = state[c]
            bit = steps - 1 - t if CHUNKS // 2 <= c < CHUNKS else t
            copy = pltpu.make_async_remote_copy(
                src_ref=box.at[(t,) + at],
                dst_ref=box_in.at[(t,) + at],
                send_sem=xs_sem.at[t, c],
                recv_sem=xr_sem.at[t, c],
                device_id=(seg_peers[bit], lat),
                device_id_type=MESH,
            )
            copy.start()
            arriving[c] = copy
            outs.append(copy)
    col = state[CHUNKS]

    stat = jnp.concatenate(state[:CHUNKS], axis=0) / n_seg
    semi_ref[...] = stat.astype(semi_ref.dtype)
    global_mean = (col / n_seg) / total_count
    row = lax.broadcasted_iota(i32, (block_size, width), 0)
    for b in range(blocks):
        block = stat[b * block_size : (b + 1) * block_size]
        block_sum = jnp.sum(jnp.where(row < cnt_ref[b], block, 0.0), axis=0, keepdims=True)
        mean = block_sum / jnp.full((1, width), cnt_ref[b], i32).astype(f32)
        excess_ref[b : b + 1, :] = mean - global_mean

    for copy in sends + back + outs:
        copy.wait_send()


def deliver(semi_ref, excess_ref, semi_out, excess_out, sem):
    copies = [
        pltpu.make_async_copy(semi_ref, semi_out, sem.at[0]),
        pltpu.make_async_copy(excess_ref, excess_out, sem.at[1]),
    ]
    for copy in copies:
        copy.start()
    for copy in copies:
        copy.wait()


def shards(n_lat, n_seg, coh_map, positions, counts):
    _, slice_bins, width = coh_map.shape
    points = positions.shape[1]
    blocks = counts.shape[0]
    slots = 2 * points // n_lat
    steps = n_seg.bit_length() - 1
    f32 = jnp.float32
    dma = pltpu.SemaphoreType.DMA
    made = pl.pallas_call(
        functools.partial(kernel, n_lat, n_seg),
        out_shape=(
            pltpu.VMEM((points, width), jnp.bfloat16),
            pltpu.VMEM((blocks, width), f32),
        ),
        in_specs=[
            pl.BlockSpec(memory_space=pl.ANY),
            pl.BlockSpec(memory_space=pl.ANY),
            pl.BlockSpec(memory_space=pl.ANY),
        ],
        out_specs=(
            pl.BlockSpec(memory_space=pltpu.VMEM),
            pl.BlockSpec(memory_space=pltpu.VMEM),
        ),
        scratch_shapes=[
            pltpu.VMEM((1, points), jnp.int32),
            pltpu.SMEM((blocks,), jnp.int32),
            pltpu.VMEM((slice_bins, width), coh_map.dtype),
            pltpu.VMEM((n_lat, 4, points), jnp.int32),
            pltpu.VMEM((n_lat, slots, width), f32),
            pltpu.VMEM((n_lat, slots, width), f32),
            pltpu.VMEM((1, width), f32),
            pltpu.VMEM((n_lat, 1, width), f32),
            pltpu.VMEM((steps, CHUNKS, points // CHUNKS, width), f32),
            pltpu.VMEM((steps, CHUNKS, points // CHUNKS, width), f32),
            pltpu.VMEM((steps, 1, width), f32),
            pltpu.VMEM((steps, 1, width), f32),
            dma((PIECES,)),
            dma((n_lat,)),
            dma((n_lat,)),
            dma((n_lat,)),
            dma((n_lat,)),
            dma((n_lat,)),
            dma((n_lat,)),
            dma((steps, CHUNKS + 1)),
            dma((steps, CHUNKS + 1)),
            dma((2,)),
        ],
        compiler_params=pltpu.CompilerParams(collective_id=0, has_side_effects=True),
    )(positions, counts, coh_map)
    made = [pltpu.with_memory_space_constraint(x, pltpu.VMEM) for x in made]
    return pl.pallas_call(
        deliver,
        out_shape=tuple(jax.ShapeDtypeStruct(x.shape, x.dtype) for x in made),
        in_specs=[pl.BlockSpec(memory_space=pltpu.VMEM)] * 2,
        out_specs=(pl.BlockSpec(memory_space=pl.ANY),) * 2,
        scratch_shapes=[dma((2,))],
    )(*made)


def solution(mesh):
    in_specs = (P("seg", "lat", None), P("seg", "lat"), P("lat"))
    out_specs = (P("lat", None), P("lat", None))
    body = functools.partial(shards, mesh.shape["lat"], mesh.shape["seg"])
    return jax.shard_map(body, mesh=mesh, in_specs=in_specs, out_specs=out_specs, check_vma=False)
```

```python
import functools

import jax
import jax.numpy as jnp
from jax import lax
from jax.experimental import pallas as pl
from jax.experimental.pallas import tpu as pltpu
from jax.sharding import PartitionSpec as P

MESH = pl.DeviceIdType.MESH
PIECES = 4
PARTS = 4


def flip(index, mask):
    out = index
    w = 1
    while w <= mask:
        if mask & w:
            out = out + w - 2 * w * lax.rem(index // w, 2)
        w *= 2
    return out


def kernel(
    n_lat,
    n_seg,
    pos_hbm,
    cnt_hbm,
    coh_hbm,
    semi_ref,
    excess_ref,
    pos_ref,
    cnt_ref,
    coh,
    gath,
    rows_out,
    rows_in,
    col_out,
    col_in,
    part,
    part_in,
    psum,
    psum_in,
    coh_sem,
    gs_sem,
    gr_sem,
    rs_sem,
    rr_sem,
    cs_sem,
    cr_sem,
    xs_sem,
    xr_sem,
    in_sem,
):
    lat = lax.axis_index("lat")
    seg = lax.axis_index("seg")
    slice_bins, width = coh.shape
    points = pos_ref.shape[1]
    blocks = cnt_ref.shape[0]
    block_size = points // blocks
    slots = 2 * points // n_lat
    total_slots = n_lat * slots
    f32, bf16, i32 = jnp.float32, jnp.bfloat16, jnp.int32

    barrier = pltpu.get_barrier_semaphore()
    lat_peers = [flip(lat, j) for j in range(n_lat)]
    far_first = list(range(n_lat - 1, 0, -1))
    for j in far_first:
        pl.semaphore_signal(barrier, inc=1, device_id=(seg, lat_peers[j]), device_id_type=MESH)
    for b in range(1, n_seg):
        pl.semaphore_signal(barrier, inc=1, device_id=(flip(seg, b), lat), device_id_type=MESH)

    small = [
        pltpu.make_async_copy(pos_hbm, pos_ref, in_sem.at[0]),
        pltpu.make_async_copy(cnt_hbm, cnt_ref, in_sem.at[1]),
    ]
    for copy in small:
        copy.start()
    piece = slice_bins // PIECES
    loads = []
    for k in range(PIECES):
        rng = pl.ds(k * piece, piece)
        loads.append(pltpu.make_async_copy(coh_hbm.at[0, rng], coh.at[rng], coh_sem.at[k]))
        loads[-1].start()
    for copy in small:
        copy.wait()

    pos = pos_ref[...]
    lane = lax.broadcasted_iota(i32, (1, points), 1)
    dest = (pos // 256) // slice_bins
    rel = jnp.bitwise_xor(dest, jnp.full((1, points), lat, i32))
    hits = lax.broadcasted_iota(i32, (n_lat, points), 0) == rel
    hits_f = hits.astype(f32)
    tri = (
        lax.broadcasted_iota(i32, (points, points), 0)
        < lax.broadcasted_iota(i32, (points, points), 1)
    ).astype(f32)
    before = jnp.dot(hits_f.astype(bf16), tri.astype(bf16), preferred_element_type=f32)
    slot = jnp.sum(before * hits_f, axis=0, keepdims=True).astype(i32)
    sid = rel * slots + slot
    limit = jnp.zeros((1, points), i32)
    for b in range(blocks):
        limit = jnp.where(lane // block_size == b, cnt_ref[b], limit)
    valid = (lane % block_size < limit).astype(i32)
    gath[0, 0:1, :] = sid
    gath[0, 1:2, :] = pos
    gath[0, 2:3, :] = valid
    gath[0, 3:4, :] = valid

    pl.semaphore_wait(barrier, n_lat - 1 + n_seg - 1)
    sends = []
    for j in far_first:
        copy = pltpu.make_async_remote_copy(
            src_ref=gath.at[0],
            dst_ref=gath.at[j],
            send_sem=gs_sem.at[j],
            recv_sem=gr_sem.at[j],
            device_id=(seg, lat_peers[j]),
            device_id_type=MESH,
        )
        copy.start()
        sends.append(copy)

    pick_t = (lax.broadcasted_iota(i32, (total_slots, points), 0) == sid).astype(f32)
    pick = pick_t.T.astype(bf16)

    arriving = {j: copy for j, copy in zip(far_first, sends)}

    pos_bits = 8
    bin_bits = (slice_bins - 1).bit_length()
    depth = min(256, slice_bins)
    depth_bits = depth.bit_length() - 1
    base = lat * (slice_bins << pos_bits)
    flag = slice_bins << pos_bits
    sub = lax.broadcasted_iota(i32, (slots, points), 0)
    group = n_lat // PARTS
    span = group * slots
    bins = lax.broadcasted_iota(i32, (span, depth), 1)
    zero = jnp.zeros((span, depth), bf16)
    per_piece = piece // depth
    count = jnp.zeros((1, points), i32)
    col = jnp.zeros((1, width), f32)
    back, col_back = [], []
    coming = {}
    for part_id in range(PARTS):
        owners = list(range(part_id * group, (part_id + 1) * group))
        cols = []
        for j in owners:
            if j > 0:
                arriving[j].wait_recv()
            live_row = gath[j, 2:3, :]
            code = (gath[j, 1:2, :] - base + flag * (1 + live_row)).astype(f32)
            here = (gath[j, 0:1, :] - j * slots) == sub
            cols.append(jnp.sum(jnp.where(here, code, 0.0), axis=1, keepdims=True))
            count = count + live_row
        code = jnp.concatenate(cols, axis=0).astype(i32)
        kind = lax.shift_right_logical(code, bin_bits + pos_bits)
        low = lax.shift_right_logical(code & (flag - 1), pos_bits)
        upper = (code & ((1 << pos_bits) - 1)).astype(f32) * (1.0 / (1 << pos_bits))
        chunk = jnp.where(kind > 0, lax.shift_right_logical(low, depth_bits), -2)
        in_chunk = low & (depth - 1)
        local = jnp.where(bins == in_chunk, 1.0 - upper, 0.0)
        local = jnp.where(bins == ((in_chunk + 1) & (depth - 1)), upper, local).astype(bf16)
        where_id = jnp.where(bins < in_chunk, chunk + 1, chunk).astype(f32).astype(bf16)
        held = jnp.zeros((span, width), f32)
        for k in range(PIECES):
            if part_id == 0:
                loads[k].wait()
            weights = jnp.concatenate(
                [
                    jnp.where(where_id == jnp.asarray(k * per_piece + c, bf16), local, zero)
                    for c in range(per_piece)
                ],
                axis=1,
            )
            held = held + jnp.dot(
                weights, coh[k * piece : (k + 1) * piece, :], preferred_element_type=f32
            )
        for i, j in enumerate(owners):
            rows_out[j] = held[i * slots : (i + 1) * slots, :]
        for j in reversed(owners):
            if j == 0:
                continue
            copy = pltpu.make_async_remote_copy(
                src_ref=rows_out.at[j],
                dst_ref=rows_in.at[j],
                send_sem=rs_sem.at[j],
                recv_sem=rr_sem.at[j],
                device_id=(seg, lat_peers[j]),
                device_id_type=MESH,
            )
            copy.start()
            back.append(copy)
            coming[j] = copy
        col = col + jnp.sum(jnp.where(kind > 1, held, 0.0), axis=0, keepdims=True)
    col_out[...] = col
    for j in far_first:
        copy = pltpu.make_async_remote_copy(
            src_ref=col_out,
            dst_ref=col_in.at[j],
            send_sem=cs_sem.at[j],
            recv_sem=cr_sem.at[j],
            device_id=(seg, lat_peers[j]),
            device_id_type=MESH,
        )
        copy.start()
        col_back.append(copy)
    total_count = jnp.sum(count.astype(f32), axis=1, keepdims=True)

    total = jnp.zeros((points, width), f32)
    for part_id in range(PARTS):
        owners = list(range(part_id * group, (part_id + 1) * group))
        got = []
        for j in owners:
            if j > 0:
                coming[j].wait_recv()
            got.append(rows_in[j] if j > 0 else rows_out[0])
        got = jnp.concatenate(got, axis=0)
        high = got.astype(bf16)
        rest = (got - high.astype(f32)).astype(bf16)
        mine = pick[:, part_id * span : (part_id + 1) * span]
        total = total + jnp.dot(
            jnp.concatenate([mine, mine], axis=1),
            jnp.concatenate([high, rest], axis=0),
            preferred_element_type=f32,
        )

    part[0] = total
    outs = []

    def tell(box, box_in, q):
        for m in range(n_seg - 1, 0, -1):
            copy = pltpu.make_async_remote_copy(
                src_ref=box.at[0],
                dst_ref=box_in.at[m],
                send_sem=xs_sem.at[m, q],
                recv_sem=xr_sem.at[m, q],
                device_id=(flip(seg, m), lat),
                device_id_type=MESH,
            )
            copy.start()
            outs.append(copy)

    def tree(terms):
        w = 1
        while w < n_seg:
            terms = [terms[i] + terms[i + 1] for i in range(0, len(terms), 2)]
            w *= 2
        return terms[0]

    tell(part, part_in, 0)
    for copy in col_back:
        copy.wait_recv()
    for j in range(1, n_lat):
        col = col + col_in[j]
    psum[0] = col
    tell(psum, psum_in, 1)
    for copy in outs:
        copy.wait_recv()
    stat = tree([total] + [part_in[m] for m in range(1, n_seg)]) / n_seg
    col = tree([col] + [psum_in[m] for m in range(1, n_seg)])
    semi_ref[...] = stat.astype(semi_ref.dtype)
    global_mean = (col / n_seg) / total_count
    row = lax.broadcasted_iota(i32, (block_size, width), 0)
    for b in range(blocks):
        block = stat[b * block_size : (b + 1) * block_size]
        block_sum = jnp.sum(jnp.where(row < cnt_ref[b], block, 0.0), axis=0, keepdims=True)
        mean = block_sum / jnp.full((1, width), cnt_ref[b], i32).astype(f32)
        excess_ref[b : b + 1, :] = mean - global_mean

    for copy in sends + back + col_back + outs:
        copy.wait_send()


def deliver(semi_ref, excess_ref, semi_out, excess_out, sem):
    copies = [
        pltpu.make_async_copy(semi_ref, semi_out, sem.at[0]),
        pltpu.make_async_copy(excess_ref, excess_out, sem.at[1]),
    ]
    for copy in copies:
        copy.start()
    for copy in copies:
        copy.wait()


def shards(n_lat, n_seg, coh_map, positions, counts):
    _, slice_bins, width = coh_map.shape
    points = positions.shape[1]
    blocks = counts.shape[0]
    slots = 2 * points // n_lat
    f32 = jnp.float32
    dma = pltpu.SemaphoreType.DMA
    made = pl.pallas_call(
        functools.partial(kernel, n_lat, n_seg),
        out_shape=(
            pltpu.VMEM((points, width), jnp.bfloat16),
            pltpu.VMEM((blocks, width), f32),
        ),
        in_specs=[
            pl.BlockSpec(memory_space=pl.ANY),
            pl.BlockSpec(memory_space=pl.ANY),
            pl.BlockSpec(memory_space=pl.ANY),
        ],
        out_specs=(
            pl.BlockSpec(memory_space=pltpu.VMEM),
            pl.BlockSpec(memory_space=pltpu.VMEM),
        ),
        scratch_shapes=[
            pltpu.VMEM((1, points), jnp.int32),
            pltpu.SMEM((blocks,), jnp.int32),
            pltpu.VMEM((slice_bins, width), coh_map.dtype),
            pltpu.VMEM((n_lat, 4, points), jnp.int32),
            pltpu.VMEM((n_lat, slots, width), f32),
            pltpu.VMEM((n_lat, slots, width), f32),
            pltpu.VMEM((1, width), f32),
            pltpu.VMEM((n_lat, 1, width), f32),
            pltpu.VMEM((n_seg, points, width), f32),
            pltpu.VMEM((n_seg, points, width), f32),
            pltpu.VMEM((n_seg, 1, width), f32),
            pltpu.VMEM((n_seg, 1, width), f32),
            dma((PIECES,)),
            dma((n_lat,)),
            dma((n_lat,)),
            dma((n_lat,)),
            dma((n_lat,)),
            dma((n_lat,)),
            dma((n_lat,)),
            dma((n_seg, 2)),
            dma((n_seg, 2)),
            dma((2,)),
        ],
        compiler_params=pltpu.CompilerParams(collective_id=0, has_side_effects=True),
    )(positions, counts, coh_map)
    made = [pltpu.with_memory_space_constraint(x, pltpu.VMEM) for x in made]
    return pl.pallas_call(
        deliver,
        out_shape=tuple(jax.ShapeDtypeStruct(x.shape, x.dtype) for x in made),
        in_specs=[pl.BlockSpec(memory_space=pltpu.VMEM)] * 2,
        out_specs=(pl.BlockSpec(memory_space=pl.ANY),) * 2,
        scratch_shapes=[dma((2,))],
    )(*made)


def solution(mesh):
    in_specs = (P("seg", "lat", None), P("seg", "lat"), P("lat"))
    out_specs = (P("lat", None), P("lat", None))
    body = functools.partial(shards, mesh.shape["lat"], mesh.shape["seg"])
    return jax.shard_map(body, mesh=mesh, in_specs=in_specs, out_specs=out_specs, check_vma=False)
```

```python
import functools

import jax
import jax.numpy as jnp
from jax import lax
from jax.experimental import pallas as pl
from jax.experimental.pallas import tpu as pltpu
from jax.sharding import PartitionSpec as P

MESH = pl.DeviceIdType.MESH
PIECES = 1
PARTS = 4
CUTS = 2


def flip(index, mask):
    out = index
    w = 1
    while w <= mask:
        if mask & w:
            out = out + w - 2 * w * lax.rem(index // w, 2)
        w *= 2
    return out


def kernel(
    n_lat,
    n_seg,
    pos_hbm,
    cnt_hbm,
    coh_hbm,
    semi_ref,
    excess_ref,
    pos_ref,
    cnt_ref,
    coh,
    gath,
    rows_out,
    rows_in,
    col_out,
    col_in,
    part,
    part_in,
    psum,
    psum_in,
    coh_sem,
    gs_sem,
    gr_sem,
    rs_sem,
    rr_sem,
    cs_sem,
    cr_sem,
    xs_sem,
    xr_sem,
    in_sem,
):
    lat = lax.axis_index("lat")
    seg = lax.axis_index("seg")
    slice_bins, width = coh.shape
    points = pos_ref.shape[1]
    blocks = cnt_ref.shape[0]
    block_size = points // blocks
    slots = 2 * points // n_lat
    total_slots = n_lat * slots
    f32, bf16, i32 = jnp.float32, jnp.bfloat16, jnp.int32

    barrier = pltpu.get_barrier_semaphore()
    lat_peers = [flip(lat, j) for j in range(n_lat)]
    far_first = list(range(n_lat - 1, 0, -1))
    for j in far_first:
        pl.semaphore_signal(barrier, inc=1, device_id=(seg, lat_peers[j]), device_id_type=MESH)
    for b in range(1, n_seg):
        pl.semaphore_signal(barrier, inc=1, device_id=(flip(seg, b), lat), device_id_type=MESH)

    small = [
        pltpu.make_async_copy(pos_hbm, pos_ref, in_sem.at[0]),
        pltpu.make_async_copy(cnt_hbm, cnt_ref, in_sem.at[1]),
    ]
    for copy in small:
        copy.start()
    piece = slice_bins // PIECES
    loads = []
    for k in range(PIECES):
        rng = pl.ds(k * piece, piece)
        loads.append(pltpu.make_async_copy(coh_hbm.at[0, rng], coh.at[rng], coh_sem.at[k]))
        loads[-1].start()
    for copy in small:
        copy.wait()

    pos = pos_ref[...]
    lane = lax.broadcasted_iota(i32, (1, points), 1)
    dest = (pos // 256) // slice_bins
    rel = jnp.bitwise_xor(dest, jnp.full((1, points), lat, i32))
    hits = lax.broadcasted_iota(i32, (n_lat, points), 0) == rel
    hits_f = hits.astype(f32)
    tri = (
        lax.broadcasted_iota(i32, (points, points), 0)
        < lax.broadcasted_iota(i32, (points, points), 1)
    ).astype(f32)
    before = jnp.dot(hits_f.astype(bf16), tri.astype(bf16), preferred_element_type=f32)
    slot = jnp.sum(before * hits_f, axis=0, keepdims=True).astype(i32)
    sid = rel * slots + slot
    limit = jnp.zeros((1, points), i32)
    for b in range(blocks):
        limit = jnp.where(lane // block_size == b, cnt_ref[b], limit)
    valid = (lane % block_size < limit).astype(i32)
    gath[0, 0:1, :] = sid
    gath[0, 1:2, :] = pos
    gath[0, 2:3, :] = valid
    gath[0, 3:4, :] = valid

    pl.semaphore_wait(barrier, n_lat - 1 + n_seg - 1)
    sends = []
    for j in far_first:
        copy = pltpu.make_async_remote_copy(
            src_ref=gath.at[0],
            dst_ref=gath.at[j],
            send_sem=gs_sem.at[j],
            recv_sem=gr_sem.at[j],
            device_id=(seg, lat_peers[j]),
            device_id_type=MESH,
        )
        copy.start()
        sends.append(copy)

    pick_t = (lax.broadcasted_iota(i32, (total_slots, points), 0) == sid).astype(f32)
    pick = pick_t.T.astype(bf16)

    arriving = {j: copy for j, copy in zip(far_first, sends)}

    pos_bits = 8
    bin_bits = (slice_bins - 1).bit_length()
    depth = min(256, slice_bins)
    depth_bits = depth.bit_length() - 1
    base = lat * (slice_bins << pos_bits)
    flag = slice_bins << pos_bits
    sub = lax.broadcasted_iota(i32, (slots, points), 0)
    group = n_lat // PARTS
    span = group * slots
    bins = lax.broadcasted_iota(i32, (span, depth), 1)
    zero = jnp.zeros((span, depth), bf16)
    per_piece = piece // depth
    count = jnp.zeros((1, points), i32)
    col = jnp.zeros((1, width), f32)
    back, col_back = [], []
    coming = {}
    for part_id in range(PARTS):
        owners = list(range(part_id * group, (part_id + 1) * group))
        cols = []
        for j in owners:
            if j > 0:
                arriving[j].wait_recv()
            live_row = gath[j, 2:3, :]
            code = (gath[j, 1:2, :] - base + flag * (1 + live_row)).astype(f32)
            here = (gath[j, 0:1, :] - j * slots) == sub
            cols.append(jnp.sum(jnp.where(here, code, 0.0), axis=1, keepdims=True))
            count = count + live_row
        code = jnp.concatenate(cols, axis=0).astype(i32)
        kind = lax.shift_right_logical(code, bin_bits + pos_bits)
        low = lax.shift_right_logical(code & (flag - 1), pos_bits)
        upper = (code & ((1 << pos_bits) - 1)).astype(f32) * (1.0 / (1 << pos_bits))
        chunk = jnp.where(kind > 0, lax.shift_right_logical(low, depth_bits), -2)
        in_chunk = low & (depth - 1)
        local = jnp.where(bins == in_chunk, 1.0 - upper, 0.0)
        local = jnp.where(bins == ((in_chunk + 1) & (depth - 1)), upper, local).astype(bf16)
        where_id = jnp.where(bins < in_chunk, chunk + 1, chunk).astype(f32).astype(bf16)
        held = jnp.zeros((span, width), f32)
        for k in range(PIECES):
            if part_id == 0:
                loads[k].wait()
            weights = jnp.concatenate(
                [
                    jnp.where(where_id == jnp.asarray(k * per_piece + c, bf16), local, zero)
                    for c in range(per_piece)
                ],
                axis=1,
            )
            held = held + jnp.dot(
                weights, coh[k * piece : (k + 1) * piece, :], preferred_element_type=f32
            )
        for i, j in enumerate(owners):
            rows_out[j] = held[i * slots : (i + 1) * slots, :]
        for j in reversed(owners):
            if j == 0:
                continue
            copy = pltpu.make_async_remote_copy(
                src_ref=rows_out.at[j],
                dst_ref=rows_in.at[j],
                send_sem=rs_sem.at[j],
                recv_sem=rr_sem.at[j],
                device_id=(seg, lat_peers[j]),
                device_id_type=MESH,
            )
            copy.start()
            back.append(copy)
            coming[j] = copy
        col = col + jnp.sum(jnp.where(kind > 1, held, 0.0), axis=0, keepdims=True)
    col_out[...] = col
    for j in far_first:
        copy = pltpu.make_async_remote_copy(
            src_ref=col_out,
            dst_ref=col_in.at[j],
            send_sem=cs_sem.at[j],
            recv_sem=cr_sem.at[j],
            device_id=(seg, lat_peers[j]),
            device_id_type=MESH,
        )
        copy.start()
        col_back.append(copy)
    total_count = jnp.sum(count.astype(f32), axis=1, keepdims=True)

    highs = []
    rests = []
    for part_id in range(PARTS):
        owners = list(range(part_id * group, (part_id + 1) * group))
        got = []
        for j in owners:
            if j > 0:
                coming[j].wait_recv()
            got.append(rows_in[j] if j > 0 else rows_out[0])
        got = jnp.concatenate(got, axis=0)
        high = got.astype(bf16)
        highs.append(high)
        rests.append((got - high.astype(f32)).astype(bf16))
    spread = jnp.concatenate(highs + rests, axis=0)
    outs = []

    def tell(src, dsts, q):
        for m in range(n_seg - 1, 0, -1):
            copy = pltpu.make_async_remote_copy(
                src_ref=src,
                dst_ref=dsts[m],
                send_sem=xs_sem.at[m, q],
                recv_sem=xr_sem.at[m, q],
                device_id=(flip(seg, m), lat),
                device_id_type=MESH,
            )
            copy.start()
            outs.append(copy)

    part_rows = points // CUTS
    for h in range(CUTS):
        rng = pl.ds(h * part_rows, part_rows)
        mine = pick[h * part_rows : (h + 1) * part_rows]
        part[0, rng] = jnp.dot(
            jnp.concatenate([mine, mine], axis=1), spread, preferred_element_type=f32
        )
        tell(part.at[0, rng], [part_in.at[m, rng] for m in range(n_seg)], h)

    def tree(terms):
        w = 1
        while w < n_seg:
            terms = [terms[i] + terms[i + 1] for i in range(0, len(terms), 2)]
            w *= 2
        return terms[0]

    for copy in col_back:
        copy.wait_recv()
    for j in range(1, n_lat):
        col = col + col_in[j]
    psum[0] = col
    tell(psum.at[0], [psum_in.at[m] for m in range(n_seg)], CUTS)
    for copy in outs:
        copy.wait_recv()
    stat = tree([part[0]] + [part_in[m] for m in range(1, n_seg)]) / n_seg
    col = tree([col] + [psum_in[m] for m in range(1, n_seg)])
    semi_ref[...] = stat.astype(semi_ref.dtype)
    global_mean = (col / n_seg) / total_count
    row = lax.broadcasted_iota(i32, (block_size, width), 0)
    for b in range(blocks):
        block = stat[b * block_size : (b + 1) * block_size]
        block_sum = jnp.sum(jnp.where(row < cnt_ref[b], block, 0.0), axis=0, keepdims=True)
        mean = block_sum / jnp.full((1, width), cnt_ref[b], i32).astype(f32)
        excess_ref[b : b + 1, :] = mean - global_mean

    for copy in sends + back + col_back + outs:
        copy.wait_send()


def deliver(semi_ref, excess_ref, semi_out, excess_out, sem):
    copies = [
        pltpu.make_async_copy(semi_ref, semi_out, sem.at[0]),
        pltpu.make_async_copy(excess_ref, excess_out, sem.at[1]),
    ]
    for copy in copies:
        copy.start()
    for copy in copies:
        copy.wait()


def shards(n_lat, n_seg, coh_map, positions, counts):
    _, slice_bins, width = coh_map.shape
    points = positions.shape[1]
    blocks = counts.shape[0]
    slots = 2 * points // n_lat
    f32 = jnp.float32
    dma = pltpu.SemaphoreType.DMA
    made = pl.pallas_call(
        functools.partial(kernel, n_lat, n_seg),
        out_shape=(
            pltpu.VMEM((points, width), jnp.bfloat16),
            pltpu.VMEM((blocks, width), f32),
        ),
        in_specs=[
            pl.BlockSpec(memory_space=pl.ANY),
            pl.BlockSpec(memory_space=pl.ANY),
            pl.BlockSpec(memory_space=pl.ANY),
        ],
        out_specs=(
            pl.BlockSpec(memory_space=pltpu.VMEM),
            pl.BlockSpec(memory_space=pltpu.VMEM),
        ),
        scratch_shapes=[
            pltpu.VMEM((1, points), jnp.int32),
            pltpu.SMEM((blocks,), jnp.int32),
            pltpu.VMEM((slice_bins, width), coh_map.dtype),
            pltpu.VMEM((n_lat, 4, points), jnp.int32),
            pltpu.VMEM((n_lat, slots, width), f32),
            pltpu.VMEM((n_lat, slots, width), f32),
            pltpu.VMEM((1, width), f32),
            pltpu.VMEM((n_lat, 1, width), f32),
            pltpu.VMEM((n_seg, points, width), f32),
            pltpu.VMEM((n_seg, points, width), f32),
            pltpu.VMEM((n_seg, 1, width), f32),
            pltpu.VMEM((n_seg, 1, width), f32),
            dma((PIECES,)),
            dma((n_lat,)),
            dma((n_lat,)),
            dma((n_lat,)),
            dma((n_lat,)),
            dma((n_lat,)),
            dma((n_lat,)),
            dma((n_seg, CUTS + 1)),
            dma((n_seg, CUTS + 1)),
            dma((2,)),
        ],
        compiler_params=pltpu.CompilerParams(collective_id=0, has_side_effects=True),
    )(positions, counts, coh_map)
    made = [pltpu.with_memory_space_constraint(x, pltpu.VMEM) for x in made]
    return pl.pallas_call(
        deliver,
        out_shape=tuple(jax.ShapeDtypeStruct(x.shape, x.dtype) for x in made),
        in_specs=[pl.BlockSpec(memory_space=pltpu.VMEM)] * 2,
        out_specs=(pl.BlockSpec(memory_space=pl.ANY),) * 2,
        scratch_shapes=[dma((2,))],
    )(*made)


def solution(mesh):
    in_specs = (P("seg", "lat", None), P("seg", "lat"), P("lat"))
    out_specs = (P("lat", None), P("lat", None))
    body = functools.partial(shards, mesh.shape["lat"], mesh.shape["seg"])
    return jax.shard_map(body, mesh=mesh, in_specs=in_specs, out_specs=out_specs, check_vma=False)
```
